512 devices in a mesh: rows: 128 (over y, z, core), grp: 4 (over x).
Axes of the slice: x: 4, y: 4, z: 16, core: 2. Of those that a mesh axis runs over, the one named last changes fastest.
Arguments:
- basis: float32 [32, 1048576], P(None, ('rows', 'grp')), may hold values from -0.0078125 to 0.0078125, as said below
- core: float32 [32, 32], replicated, may hold values from -0.3 to 4
- snapshots: bfloat16 [4, 32, 1048576], P(None, 'grp', 'rows'), may hold values from -16 to 16
Outputs:
- new_basis: float32 [32, 1048576], P(None, ('rows', 'grp'))
- new_core: float32 [32, 32], replicated
- first_coeffs: float32 [4, 32, 32], replicated
The draws below stay inside these ranges and needn't reach their ends.
Inputs may be any that keep to these rules, and one draw needn't show every extreme that they name: `basis`: rows orthonormal up to float32 rounding.
All inputs are finite; a program needn't handle non-finite values.
Results may differ from the reference program's by a relative error of at most 0.0003.
Values may be sent and summed in bfloat16 or wider, within the bound.
No kernel may reach another device: no remote copies, remote signals or barrier semaphores. Data moves between devices by JAX's collectives and lax.ppermute only.
A program may use at most 64 MiB of HBM per device.

```python
import jax
import jax.numpy as jnp
from jax import lax

RANK = 32
COLS = 32
BATCHES = 4
NDOF = 1048576


def basis_rows(key):
    return jnp.clip(jax.random.normal(jax.random.fold_in(key, 11), (RANK, NDOF), jnp.float32), -4.0, 4.0)


def shared_row(key):
    return jnp.clip(jax.random.normal(jax.random.fold_in(key, 12), (1, NDOF), jnp.float32), -4.0, 4.0)


def cholesky_pass(vectors):
    gram = lax.dot_general(vectors, vectors, (((1,), (1,)), ((), ())), precision=lax.Precision.HIGHEST, preferred_element_type=jnp.float32)
    factor = jnp.linalg.cholesky(gram)
    return lax.linalg.triangular_solve(factor, vectors, left_side=True, lower=True)


def draw_basis(key, part):
    vectors = basis_rows(key)
    return cholesky_pass(cholesky_pass(vectors))


def draw_core(key, part):
    logs = jax.random.uniform(jax.random.fold_in(key, 21), (RANK,), jnp.float32, jnp.log(0.5), jnp.log(2.0))
    below = jax.random.uniform(jax.random.fold_in(key, 22), (RANK, RANK), jnp.float32, -0.3, 0.3)
    return jnp.diag(jnp.exp(logs)) + jnp.tril(below, -1)


def draw_snapshots(key, part):
    vectors = basis_rows(key)
    shared = shared_row(key)
    weights = jax.random.normal(jax.random.fold_in(key, 13), (BATCHES * COLS, RANK), jnp.float32)
    spread = jnp.exp(jax.random.uniform(jax.random.fold_in(key, 14), (1, RANK), jnp.float32, jnp.log(0.3), jnp.log(3.0)))
    position = jnp.arange(NDOF, dtype=jnp.float32) / (NDOF - 1.0)
    noise = jax.random.normal(jax.random.fold_in(key, 15), (BATCHES * COLS, NDOF), jnp.float32)
    ramp = 1.0 + 2.0 * position
    values = (jnp.dot(weights * spread, vectors) + 0.5 * shared + 2.0 * noise) / 4.0
    values = jnp.clip(values * ramp[None, :], -16.0, 16.0)
    return values.reshape(BATCHES, COLS, NDOF).astype(jnp.bfloat16)


def setup_inputs(seed: int = 0) -> dict:
    keys = jax.random.split(jax.random.key(seed), 4)
    basis = draw_basis(jax.random.fold_in(keys[3], 71), 0)
    core = draw_core(jax.random.fold_in(keys[3], 71), 0)
    snapshots = draw_snapshots(jax.random.fold_in(keys[3], 71), 0)
    return dict(basis=basis, core=core, snapshots=snapshots)


epsilon = 1e-06

def contract_rows(left, right):
    return lax.dot_general(left.astype(jnp.float32), right.astype(jnp.float32), (((1,), (1,)), ((), ())), precision=lax.Precision.HIGHEST, preferred_element_type=jnp.float32)

def matmul(left, right):
    return jnp.dot(left.astype(jnp.float32), right.astype(jnp.float32), precision=lax.Precision.HIGHEST, preferred_element_type=jnp.float32)

def lower_solve(factor, right):
    return lax.linalg.triangular_solve(factor, right, left_side=True, lower=True)

def small_update(core_now, total, lower):
    rank = core_now.shape[0]
    cols = lower.shape[0]
    top = jnp.concatenate([core_now, total], axis=1)
    bottom = jnp.concatenate([jnp.zeros((cols, rank), jnp.float32), lower.T], axis=1)
    stacked = jnp.concatenate([top, bottom], axis=0)
    moment = matmul(stacked, stacked.T)
    leading = moment[:, :rank]
    factor = jnp.linalg.cholesky(matmul(leading.T, leading))
    rotation = lower_solve(factor, leading.T).T
    fresh_core = jnp.linalg.cholesky(matmul(rotation.T, matmul(moment, rotation)))
    return (rotation, fresh_core)

def reference(basis, core, snapshots):
    basis_now = basis
    core_now = core
    rank = basis.shape[0]
    firsts = []
    for batch in range(BATCHES):
        raw = snapshots[batch].astype(jnp.float32)
        squares = lax.optimization_barrier(jnp.sum(raw * raw, axis=1))
        scaled = raw * lax.rsqrt(squares + epsilon)[:, None]
        first = contract_rows(basis_now, scaled)
        firsts.append(first)
        once = scaled - matmul(first.T, basis_now)
        second = contract_rows(basis_now, once)
        twice = once - matmul(second.T, basis_now)
        total = first + second
        gram = contract_rows(twice, twice)
        lower = jnp.linalg.cholesky(gram)
        fresh = lower_solve(lower, twice)
        rotation, core_now = small_update(core_now, total, lower)
        basis_now = matmul(rotation[:rank].T, basis_now) + matmul(rotation[rank:].T, fresh)
    return (basis_now, core_now, jnp.stack(firsts, axis=0))
```

```python
import jax
import jax.numpy as jnp
from jax import lax
from jax.experimental import pallas as pl
from jax.experimental.pallas import tpu as pltpu
from jax.sharding import Mesh
from jax.sharding import PartitionSpec as P

BATCHES = 4
ROWS_GRP = ("rows_0", "rows_1", "rows_2", "grp")
ROWS = ("rows_0", "rows_1", "rows_2")
NEAR = ("rows_0", "rows_2", "grp")
FAR = "rows_1"
LANES = 128
SUB = 8

epsilon = 1e-06


def exchange(parts, axis):
    return lax.all_to_all(parts, axis, split_axis=0, concat_axis=0, tiled=True)


def total_over_all(packed):
    near = lax.axis_size(NEAR)
    far = lax.axis_size(FAR)
    rows, lanes = packed.shape
    piece = exchange(packed.reshape(near, rows // near, lanes), NEAR).sum(axis=0)
    piece = exchange(jnp.broadcast_to(piece, (far, *piece.shape)), FAR).sum(axis=0)
    return exchange(jnp.broadcast_to(piece, (near, *piece.shape)), NEAR).reshape(rows, lanes)


def dot(left, right, contract=(1, 0)):
    return lax.dot_general(
        left,
        right,
        (((contract[0],), (contract[1],)), ((), ())),
        precision=lax.Precision.HIGHEST,
        preferred_element_type=jnp.float32,
    )


def dot_short(left, right, contract=(1, 0)):
    return lax.dot_general(
        left,
        right,
        (((contract[0],), (contract[1],)), ((), ())),
        preferred_element_type=jnp.float32,
    )


def three_parts(values):
    high = values.astype(jnp.bfloat16)
    rest = values - high.astype(jnp.float32)
    middle = rest.astype(jnp.bfloat16)
    low = (rest - middle.astype(jnp.float32)).astype(jnp.bfloat16)
    return high, middle, low


def by_batch(received):
    groups, batches, cols, dofs = received.shape
    return [
        jnp.concatenate([received[g, b] for g in range(groups)], axis=0) for b in range(batches)
    ]


def gram_kernel(received_ref, basis_ref, packed_ref):
    raw = jnp.concatenate(by_batch(received_ref[...]), axis=0)
    parts = jnp.concatenate(three_parts(basis_ref[...]), axis=0)
    cols = raw.shape[0]
    rank = basis_ref.shape[0]
    raw_gram = dot_short(raw, raw, (1, 1))
    cross = dot_short(parts, raw, (1, 1))
    square = dot_short(parts, parts, (1, 1))
    cross = cross[2 * rank :] + cross[rank : 2 * rank] + cross[:rank]
    square = square[2 * rank :] + square[rank : 2 * rank] + square[:rank]
    square = square[:, 2 * rank :] + square[:, rank : 2 * rank] + square[:, :rank]
    step = cols // BATCHES
    packed_ref[0:step] = raw_gram[0:step]
    packed_ref[step : 2 * step] = jnp.concatenate(
        [raw_gram[3 * step :, 3 * step :], raw_gram[step : 2 * step, step:]], axis=1
    )
    packed_ref[2 * step : 3 * step] = jnp.concatenate(
        [square, raw_gram[2 * step : 3 * step, step:]], axis=1
    )
    packed_ref[3 * step :] = cross


def eliminate(matrix, want_inverse):
    order = matrix.shape[0]
    tiles = order // SUB
    work = [matrix[SUB * g : SUB * g + SUB] for g in range(tiles)]
    row = lax.broadcasted_iota(jnp.int32, (SUB, order), 0)
    lane = lax.broadcasted_iota(jnp.int32, (SUB, order), 1)
    inverse = [jnp.where(row + SUB * g == lane, 1.0, 0.0) for g in range(tiles)]
    lower = [jnp.zeros((SUB, order), jnp.float32) for g in range(tiles)]

    def spread(tile, k):
        return jnp.broadcast_to(tile[k : k + 1], (SUB, order))

    for p in range(tiles):
        columns = {
            (m, g): jnp.broadcast_to(work[g][:, SUB * p + m : SUB * p + m + 1], (SUB, order))
            for m in range(SUB)
            for g in range(p, tiles)
        }
        scale = jnp.zeros((SUB, order), jnp.float32)
        for k in range(SUB):
            pivot = spread(columns[k, p], k)
            root = lax.rsqrt(pivot)
            recip = 1.0 / pivot
            scale = jnp.where(row == k, root, scale)
            factors = {g: columns[k, g] * recip for g in range(p, tiles)}
            factors[p] = jnp.where(row > k, factors[p], 0.0)
            if not want_inverse:
                for g in range(p, tiles):
                    part = columns[k, g] * root
                    if g == p:
                        part = jnp.where(row >= k, part, 0.0)
                    lower[g] = jnp.where(lane == SUB * p + k, part, lower[g])
            for m in range(k + 1, SUB):
                top = spread(columns[m, p], k)
                for g in range(p, tiles):
                    columns[m, g] = columns[m, g] - factors[g] * top
            top = spread(work[p], k)
            for g in range(p + 1, tiles):
                work[g] = work[g] - factors[g] * top
            work[p] = work[p] - factors[p] * top
            if want_inverse:
                top = spread(inverse[p], k)
                for g in range(p, tiles):
                    inverse[g] = inverse[g] - factors[g] * top
        if want_inverse:
            inverse[p] = inverse[p] * scale
    return jnp.concatenate(inverse if want_inverse else lower, axis=0)


def unpacked(packed, cols):
    step = cols // BATCHES
    rank = packed.shape[0] - 3 * step
    row = lax.broadcasted_iota(jnp.int32, packed.shape, 0)
    lane = lax.broadcasted_iota(jnp.int32, packed.shape, 1)
    own = jnp.where(row == lane, packed, 0.0)[: 3 * step]
    last = jnp.where(row - step == lane, packed, 0.0)[step : 2 * step, :step]
    across = jnp.concatenate(
        [jnp.sum(own, axis=0, keepdims=True)[:, : 3 * step], jnp.sum(last, axis=0, keepdims=True)],
        axis=1,
    )
    across = lax.rsqrt(across + epsilon)
    down = [jnp.sum(own[step * b : step * b + step], axis=1, keepdims=True) for b in range(3)]
    down = [lax.rsqrt(d + epsilon) for d in down + [jnp.sum(last, axis=1, keepdims=True)]]
    rows = [packed[step * b : step * b + step] * across * down[b] for b in range(3)]
    grams = [rows[b][:, step * b : step * b + step] for b in range(3)]
    grams.append(packed[step : 2 * step, :step] * across[:, 3 * step :] * down[3])
    cross = packed[3 * step :] * across
    return cross, packed[2 * step : 3 * step, :rank], rows, grams, across


def update_kernel(packed_ref, core_ref, basis_ref, received_ref, new_basis_ref, new_core_ref, firsts_ref):
    received = received_ref[...]
    cols = received.shape[0] * received.shape[1] * received.shape[2]
    step = cols // BATCHES
    cross, gram_basis, rows, grams, across = unpacked(packed_ref[...], cols)
    root = core_ref[...]
    energy = dot(root, root, (1, 1))
    of_basis = None
    of_raw = None
    for b in range(BATCHES):
        first = cross[:, step * b : step * b + step]
        firsts_ref[b] = first
        second = first - dot(gram_basis, first)
        total = first + second
        rest = first - dot(gram_basis, total)
        gram = grams[b] - dot(first, total, (0, 0)) - dot(total, rest, (0, 0))
        leading = energy + dot(total, total, (1, 1))
        total_gram = dot(total, gram)
        square = dot(leading, leading) + dot(total_gram, total, (1, 1))
        tail = dot(leading, total)
        inverse = eliminate(square, True)
        from_old = dot(inverse, energy)
        from_new = dot(inverse, total)
        root = dot(inverse, dot(leading, root))
        tail = dot(inverse, tail) + dot(inverse, total_gram)
        energy = dot(root, root, (1, 1)) + dot(tail, tail, (1, 1))
        if b + 1 < BATCHES:
            root = jnp.concatenate([root, tail], axis=1)
            left = dot(from_old, gram_basis) + dot(from_new, first, (1, 1))
            right = dot(from_old, first) + dot(from_new, grams[b])
            gram_basis = dot(left, from_old, (1, 1)) + dot(right, from_new, (1, 1))
            cross = dot(from_old, cross) + dot(from_new, rows[b])
        if b == 0:
            of_basis = from_old
            of_raw = from_new
        else:
            of_basis = dot(from_old, of_basis)
            of_raw = jnp.concatenate([dot(from_old, of_raw), from_new], axis=1)
    new_core_ref[...] = eliminate(energy, False)
    of_raw = of_raw * across
    raw = jnp.concatenate(by_batch(received), axis=0)
    parts = dot_short(jnp.concatenate(three_parts(of_raw), axis=0), raw)
    rank = of_raw.shape[0]
    new_basis_ref[...] = (
        dot(of_basis, basis_ref[...]) + parts[2 * rank :] + parts[rank : 2 * rank] + parts[:rank]
    )


def body(basis, core, snapshots):
    batches, mine, dofs = snapshots.shape
    grp = lax.axis_size("grp")
    rank = basis.shape[0]
    cols = grp * mine
    pieces = snapshots.reshape(batches, mine, grp, dofs // grp).transpose(2, 0, 1, 3)
    received = exchange(pieces, "grp")
    packed = pl.pallas_call(
        gram_kernel, out_shape=jax.ShapeDtypeStruct((3 * cols + rank, LANES), jnp.float32)
    )(received, basis)
    packed = total_over_all(packed)
    return pl.pallas_call(
        update_kernel,
        out_shape=(
            jax.ShapeDtypeStruct(basis.shape, jnp.float32),
            jax.ShapeDtypeStruct(core.shape, jnp.float32),
            jax.ShapeDtypeStruct((batches, rank, cols), jnp.float32),
        ),
    )(packed, core, basis, received)


def solution(mesh):
    finer = Mesh(
        mesh.devices.reshape(4, 16, 2, mesh.shape["grp"]), ("rows_0", "rows_1", "rows_2", "grp")
    )
    return jax.shard_map(
        body,
        mesh=finer,
        in_specs=(P(None, ROWS_GRP), P(), P(None, "grp", ROWS)),
        out_specs=(P(None, ROWS_GRP), P(), P()),
        check_vma=False,
    )
```

```python
import jax
import jax.numpy as jnp
from jax import lax
from jax.experimental import pallas as pl
from jax.experimental.pallas import tpu as pltpu
from jax.sharding import Mesh
from jax.sharding import PartitionSpec as P

BATCHES = 4
ROWS_GRP = ("rows_0", "rows_1", "rows_2", "grp")
ROWS = ("rows_0", "rows_1", "rows_2")
NEAR = ("rows_0", "rows_2", "grp")
FAR = "rows_1"
LANES = 128
SUB = 8
SMALL_GRANT = pltpu.CompilerParams(vmem_limit_bytes=8 * 2**20)

epsilon = 1e-06


def exchange(parts, axis):
    return lax.all_to_all(parts, axis, split_axis=0, concat_axis=0, tiled=True)


def total_over_all(packed):
    near = lax.axis_size(NEAR)
    far = lax.axis_size(FAR)
    rows, lanes = packed.shape
    piece = exchange(packed.reshape(near, rows // near, lanes), NEAR).sum(axis=0)
    piece = exchange(jnp.broadcast_to(piece, (far, *piece.shape)), FAR).sum(axis=0)
    return exchange(jnp.broadcast_to(piece, (near, *piece.shape)), NEAR).reshape(rows, lanes)


def dot(left, right, contract=(1, 0)):
    return lax.dot_general(
        left,
        right,
        (((contract[0],), (contract[1],)), ((), ())),
        precision=lax.Precision.HIGHEST,
        preferred_element_type=jnp.float32,
    )


def dot_short(left, right, contract=(1, 0)):
    return lax.dot_general(
        left,
        right,
        (((contract[0],), (contract[1],)), ((), ())),
        preferred_element_type=jnp.float32,
    )


def three_parts(values):
    high = values.astype(jnp.bfloat16)
    rest = values - high.astype(jnp.float32)
    middle = rest.astype(jnp.bfloat16)
    low = (rest - middle.astype(jnp.float32)).astype(jnp.bfloat16)
    return high, middle, low


def by_batch(received):
    groups, batches, cols, dofs = received.shape
    return [
        jnp.concatenate([received[g, b] for g in range(groups)], axis=0) for b in range(batches)
    ]


def gram_kernel(received_ref, basis_ref, packed_ref):
    raw = jnp.concatenate(by_batch(received_ref[...]), axis=0)
    parts = jnp.concatenate(three_parts(basis_ref[...]), axis=0)
    cols = raw.shape[0]
    rank = basis_ref.shape[0]
    raw_gram = dot_short(raw, raw, (1, 1))
    cross = dot_short(parts, raw, (1, 1))
    square = dot_short(parts, parts, (1, 1))
    cross = cross[2 * rank :] + cross[rank : 2 * rank] + cross[:rank]
    square = square[2 * rank :] + square[rank : 2 * rank] + square[:rank]
    square = square[:, 2 * rank :] + square[:, rank : 2 * rank] + square[:, :rank]
    step = cols // BATCHES
    packed_ref[0:step] = raw_gram[0:step]
    packed_ref[step : 2 * step] = jnp.concatenate(
        [raw_gram[3 * step :, 3 * step :], raw_gram[step : 2 * step, step:]], axis=1
    )
    packed_ref[2 * step : 3 * step] = jnp.concatenate(
        [square, raw_gram[2 * step : 3 * step, step:]], axis=1
    )
    packed_ref[3 * step :] = cross


def eliminate(matrix, want_inverse):
    order = matrix.shape[0]
    tiles = order // SUB
    work = [matrix[SUB * g : SUB * g + SUB] for g in range(tiles)]
    row = lax.broadcasted_iota(jnp.int32, (SUB, order), 0)
    lane = lax.broadcasted_iota(jnp.int32, (SUB, order), 1)
    inverse = [jnp.where(row + SUB * g == lane, 1.0, 0.0) for g in range(tiles)]
    lower = [jnp.zeros((SUB, order), jnp.float32) for g in range(tiles)]

    def spread(tile, k):
        return jnp.broadcast_to(tile[k : k + 1], (SUB, order))

    for p in range(tiles):
        columns = {
            (m, g): jnp.broadcast_to(work[g][:, SUB * p + m : SUB * p + m + 1], (SUB, order))
            for m in range(SUB)
            for g in range(p, tiles)
        }
        scale = jnp.zeros((SUB, order), jnp.float32)
        for k in range(SUB):
            pivot = spread(columns[k, p], k)
            root = lax.rsqrt(pivot)
            recip = 1.0 / pivot
            scale = jnp.where(row == k, root, scale)
            factors = {g: columns[k, g] * recip for g in range(p, tiles)}
            factors[p] = jnp.where(row > k, factors[p], 0.0)
            if not want_inverse:
                for g in range(p, tiles):
                    part = columns[k, g] * root
                    if g == p:
                        part = jnp.where(row >= k, part, 0.0)
                    lower[g] = jnp.where(lane == SUB * p + k, part, lower[g])
            for m in range(k + 1, SUB):
                top = spread(columns[m, p], k)
                for g in range(p, tiles):
                    columns[m, g] = columns[m, g] - factors[g] * top
            top = spread(work[p], k)
            for g in range(p + 1, tiles):
                work[g] = work[g] - factors[g] * top
            work[p] = work[p] - factors[p] * top
            if want_inverse:
                top = spread(inverse[p], k)
                for g in range(p, tiles):
                    inverse[g] = inverse[g] - factors[g] * top
        if want_inverse:
            inverse[p] = inverse[p] * scale
    return jnp.concatenate(inverse if want_inverse else lower, axis=0)


def unpacked(packed, cols):
    step = cols // BATCHES
    rank = packed.shape[0] - 3 * step
    row = lax.broadcasted_iota(jnp.int32, packed.shape, 0)
    lane = lax.broadcasted_iota(jnp.int32, packed.shape, 1)
    own = jnp.where(row == lane, packed, 0.0)[: 3 * step]
    last = jnp.where(row - step == lane, packed, 0.0)[step : 2 * step, :step]
    across = jnp.concatenate(
        [jnp.sum(own, axis=0, keepdims=True)[:, : 3 * step], jnp.sum(last, axis=0, keepdims=True)],
        axis=1,
    )
    across = lax.rsqrt(across + epsilon)
    down = [jnp.sum(own[step * b : step * b + step], axis=1, keepdims=True) for b in range(3)]
    down = [lax.rsqrt(d + epsilon) for d in down + [jnp.sum(last, axis=1, keepdims=True)]]
    rows = [packed[step * b : step * b + step] * across * down[b] for b in range(3)]
    grams = [rows[b][:, step * b : step * b + step] for b in range(3)]
    grams.append(packed[step : 2 * step, :step] * across[:, 3 * step :] * down[3])
    cross = packed[3 * step :] * across
    return cross, packed[2 * step : 3 * step, :rank], rows, grams, across


def update_kernel(packed_ref, core_ref, basis_ref, received_ref, new_basis_ref, new_core_ref, firsts_ref):
    received = received_ref[...]
    cols = received.shape[0] * received.shape[1] * received.shape[2]
    step = cols // BATCHES
    cross, gram_basis, rows, grams, across = unpacked(packed_ref[...], cols)
    root = core_ref[...]
    energy = dot(root, root, (1, 1))
    of_basis = None
    of_raw = None
    for b in range(BATCHES):
        first = cross[:, step * b : step * b + step]
        firsts_ref[b] = first
        second = first - dot(gram_basis, first)
        total = first + second
        rest = first - dot(gram_basis, total)
        gram = grams[b] - dot(first, total, (0, 0)) - dot(total, rest, (0, 0))
        leading = energy + dot(total, total, (1, 1))
        total_gram = dot(total, gram)
        square = dot(leading, leading) + dot(total_gram, total, (1, 1))
        tail = dot(leading, total)
        inverse = eliminate(square, True)
        from_old = dot(inverse, energy)
        from_new = dot(inverse, total)
        root = dot(inverse, dot(leading, root))
        tail = dot(inverse, tail) + dot(inverse, total_gram)
        energy = dot(root, root, (1, 1)) + dot(tail, tail, (1, 1))
        if b + 1 < BATCHES:
            root = jnp.concatenate([root, tail], axis=1)
            left = dot(from_old, gram_basis) + dot(from_new, first, (1, 1))
            right = dot(from_old, first) + dot(from_new, grams[b])
            gram_basis = dot(left, from_old, (1, 1)) + dot(right, from_new, (1, 1))
            cross = dot(from_old, cross) + dot(from_new, rows[b])
        if b == 0:
            of_basis = from_old
            of_raw = from_new
        else:
            of_basis = dot(from_old, of_basis)
            of_raw = jnp.concatenate([dot(from_old, of_raw), from_new], axis=1)
    new_core_ref[...] = eliminate(energy, False)
    of_raw = of_raw * across
    raw = jnp.concatenate(by_batch(received), axis=0)
    parts = dot_short(jnp.concatenate(three_parts(of_raw), axis=0), raw)
    rank = of_raw.shape[0]
    new_basis_ref[...] = (
        dot(of_basis, basis_ref[...]) + parts[2 * rank :] + parts[rank : 2 * rank] + parts[:rank]
    )


def body(basis, core, snapshots):
    batches, mine, dofs = snapshots.shape
    grp = lax.axis_size("grp")
    rank = basis.shape[0]
    cols = batches * grp * mine
    pieces = snapshots.reshape(batches, mine, grp, dofs // grp).transpose(2, 0, 1, 3)
    received = exchange(pieces, "grp")
    packed = pl.pallas_call(
        gram_kernel,
        out_shape=jax.ShapeDtypeStruct((3 * (cols // batches) + rank, LANES), jnp.float32),
        compiler_params=SMALL_GRANT,
    )(received, basis)
    packed = total_over_all(packed)
    return pl.pallas_call(
        update_kernel,
        out_shape=(
            jax.ShapeDtypeStruct(basis.shape, jnp.float32),
            jax.ShapeDtypeStruct(core.shape, jnp.float32),
            jax.ShapeDtypeStruct((batches, rank, cols // batches), jnp.float32),
        ),
        compiler_params=SMALL_GRANT,
    )(packed, core, basis, received)


def solution(mesh):
    finer = Mesh(
        mesh.devices.reshape(4, 16, 2, mesh.shape["grp"]), ("rows_0", "rows_1", "rows_2", "grp")
    )
    return jax.shard_map(
        body,
        mesh=finer,
        in_specs=(P(None, ROWS_GRP), P(), P(None, "grp", ROWS)),
        out_specs=(P(None, ROWS_GRP), P(), P()),
        check_vma=False,
    )
```

```python
import jax
import jax.numpy as jnp
from jax import lax
from jax.experimental import pallas as pl
from jax.experimental.pallas import tpu as pltpu
from jax.sharding import Mesh
from jax.sharding import PartitionSpec as P

BATCHES = 4
ROWS_GRP = ("rows_0", "rows_1", "rows_2", "grp")
ROWS = ("rows_0", "rows_1", "rows_2")
NEAR = ("rows_0", "rows_2", "grp")
FAR = "rows_1"
LANES = 128
SUB = 8
SMALL_GRANT = pltpu.CompilerParams(vmem_limit_bytes=8 * 2**20)

epsilon = 1e-06


def exchange(parts, axis):
    return lax.all_to_all(parts, axis, split_axis=0, concat_axis=0, tiled=True)


def total_over_all(packed):
    near = lax.axis_size(NEAR)
    far = lax.axis_size(FAR)
    rows, lanes = packed.shape
    piece = exchange(packed.reshape(near, rows // near, lanes), NEAR).sum(axis=0)
    piece = exchange(jnp.broadcast_to(piece, (far, *piece.shape)), FAR).sum(axis=0)
    return exchange(jnp.broadcast_to(piece, (near, *piece.shape)), NEAR).reshape(rows, lanes)


def dot(left, right, contract=(1, 0)):
    return lax.dot_general(
        left,
        right,
        (((contract[0],), (contract[1],)), ((), ())),
        precision=lax.Precision.HIGHEST,
        preferred_element_type=jnp.float32,
    )


def dot_short(left, right, contract=(1, 0)):
    return lax.dot_general(
        left,
        right,
        (((contract[0],), (contract[1],)), ((), ())),
        preferred_element_type=jnp.float32,
    )


def three_parts(values):
    high = values.astype(jnp.bfloat16)
    rest = values - high.astype(jnp.float32)
    middle = rest.astype(jnp.bfloat16)
    low = (rest - middle.astype(jnp.float32)).astype(jnp.bfloat16)
    return high, middle, low


def by_batch(received):
    groups, batches, cols, dofs = received.shape
    return [
        jnp.concatenate([received[g, b] for g in range(groups)], axis=0) for b in range(batches)
    ]


def gram_kernel(received_ref, basis_ref, packed_ref):
    raw = jnp.concatenate(by_batch(received_ref[...]), axis=0)
    parts = jnp.concatenate(three_parts(basis_ref[...]), axis=0)
    cols = raw.shape[0]
    rank = basis_ref.shape[0]
    raw_gram = dot_short(raw, raw, (1, 1))
    cross = dot_short(parts, raw, (1, 1))
    square = dot_short(parts, parts, (1, 1))
    cross = cross[2 * rank :] + cross[rank : 2 * rank] + cross[:rank]
    square = square[2 * rank :] + square[rank : 2 * rank] + square[:rank]
    square = square[:, 2 * rank :] + square[:, rank : 2 * rank] + square[:, :rank]
    step = cols // BATCHES
    packed_ref[0:step] = raw_gram[0:step]
    packed_ref[step : 2 * step] = jnp.concatenate(
        [raw_gram[3 * step :, 3 * step :], raw_gram[step : 2 * step, step:]], axis=1
    )
    packed_ref[2 * step : 3 * step] = jnp.concatenate(
        [square, raw_gram[2 * step : 3 * step, step:]], axis=1
    )
    packed_ref[3 * step :] = cross


def eliminate(matrix, want_inverse):
    order = matrix.shape[0]
    tiles = order // SUB
    work = [matrix[SUB * g : SUB * g + SUB] for g in range(tiles)]
    row = lax.broadcasted_iota(jnp.int32, (SUB, order), 0)
    lane = lax.broadcasted_iota(jnp.int32, (SUB, order), 1)
    inverse = [jnp.where(row + SUB * g == lane, 1.0, 0.0) for g in range(tiles)]
    lower = [jnp.zeros((SUB, order), jnp.float32) for g in range(tiles)]

    def spread(tile, k):
        return jnp.broadcast_to(tile[k : k + 1], (SUB, order))

    for p in range(tiles):
        columns = {
            (m, g): jnp.broadcast_to(work[g][:, SUB * p + m : SUB * p + m + 1], (SUB, order))
            for m in range(SUB)
            for g in range(p, tiles)
        }
        scale = jnp.zeros((SUB, order), jnp.float32)
        for k in range(SUB):
            pivot = spread(columns[k, p], k)
            root = lax.rsqrt(pivot)
            recip = 1.0 / pivot
            scale = jnp.where(row == k, root, scale)
            factors = {g: columns[k, g] * recip for g in range(p, tiles)}
            factors[p] = jnp.where(row > k, factors[p], 0.0)
            if not want_inverse:
                for g in range(p, tiles):
                    part = columns[k, g] * root
                    if g == p:
                        part = jnp.where(row >= k, part, 0.0)
                    lower[g] = jnp.where(lane == SUB * p + k, part, lower[g])
            for m in range(k + 1, SUB):
                top = spread(columns[m, p], k)
                for g in range(p, tiles):
                    columns[m, g] = columns[m, g] - factors[g] * top
            top = spread(work[p], k)
            for g in range(p + 1, tiles):
                work[g] = work[g] - factors[g] * top
            work[p] = work[p] - factors[p] * top
            if want_inverse:
                top = spread(inverse[p], k)
                for g in range(p, tiles):
                    inverse[g] = inverse[g] - factors[g] * top
        if want_inverse:
            inverse[p] = inverse[p] * scale
    return jnp.concatenate(inverse if want_inverse else lower, axis=0)


def update_kernel(
    packed_ref, core_ref, basis_ref, received_ref, new_basis_ref, new_core_ref, firsts_ref, made_ref, sent
):
    cols = packed_ref.shape[1]
    step = cols // BATCHES
    rank = core_ref.shape[0]
    eye = jnp.where(
        lax.broadcasted_iota(jnp.int32, (step, step), 0) == lax.broadcasted_iota(jnp.int32, (step, step), 1), 1.0, 0.0
    )
    rows = [packed_ref[step * b : step * b + step] for b in range(BATCHES - 1)]
    cross = packed_ref[3 * step :]
    grams = [rows[b][:, step * b : step * b + step] for b in range(BATCHES - 1)] + [rows[1][:, :step]]
    scales = [lax.rsqrt(jnp.sum(g * eye, axis=0, keepdims=True) + epsilon) for g in grams]
    gram_basis = rows[2][:, :rank]
    first = cross[:, :step] * scales[0]
    root = core_ref[...]
    energy = dot(root, root, (1, 1))
    of_basis = None
    of_raw = None
    for b in range(BATCHES):
        more = b + 1 < BATCHES
        scale = scales[b]
        firsts_ref[b] = first
        defect = eye - gram_basis
        second = dot(defect, first)
        total = first + second
        weight = total * scale
        rest = dot(defect, second)
        minus_square = dot(-total, total, (1, 1))
        total_raw = dot(weight, grams[b]) * scale
        total_gram = (
            total_raw - dot(dot(total, first, (1, 1)), total) + dot(minus_square, rest)
        )
        leading = energy - minus_square
        square = dot(leading, leading) + dot(total_gram, total, (1, 1))
        tail = dot(leading, total)
        grown = dot(leading, root)
        if more:
            mixed = dot(energy, cross) - dot(-weight, rows[b])
            upcoming = mixed[:, step * b + step : step * b + 2 * step]
            held = dot(energy, first)
            mixed_gram = (
                dot(dot(energy, gram_basis), energy)
                + dot(held, total, (1, 1))
                + dot(total, held, (1, 1))
                + dot(total_raw, total, (1, 1))
            )
        if b:
            of_basis = dot(energy, of_basis)
            of_raw = jnp.concatenate([dot(energy, of_raw), weight], axis=1)
        else:
            of_basis = energy
            of_raw = weight
        inverse = eliminate(square, True)
        root = dot(inverse, grown)
        tail = dot(inverse, tail) + dot(inverse, total_gram)
        if more:
            first = dot(inverse, upcoming) * scales[b + 1]
            gram_basis = dot(dot(inverse, mixed_gram), inverse, (1, 1))
            cross = dot(inverse, mixed)
        energy = dot(root, root, (1, 1)) + dot(tail, tail, (1, 1))
        if more:
            root = jnp.concatenate([root, tail], axis=1)
        of_basis = dot(inverse, of_basis)
        of_raw = dot(inverse, of_raw)
    raw = jnp.concatenate(by_batch(received_ref[...]), axis=0)
    parts = dot_short(jnp.concatenate(three_parts(of_raw), axis=0), raw)
    made_ref[...] = (
        dot(of_basis, basis_ref[...]) + parts[2 * rank :] + parts[rank : 2 * rank] + parts[:rank]
    )
    out = pltpu.make_async_copy(made_ref, new_basis_ref, sent)
    out.start()
    new_core_ref[...] = eliminate(energy, False)
    out.wait()


def gram_call(received, basis):
    groups, batches, mine, dofs = received.shape
    return pl.pallas_call(
        gram_kernel,
        out_shape=jax.ShapeDtypeStruct((3 * groups * mine + basis.shape[0], LANES), jnp.float32),
        compiler_params=SMALL_GRANT,
    )(received, basis)


def update_call(packed, core, basis, received):
    groups, batches, mine, dofs = received.shape
    rank = basis.shape[0]
    return pl.pallas_call(
        update_kernel,
        out_shape=(
            jax.ShapeDtypeStruct(basis.shape, jnp.float32),
            jax.ShapeDtypeStruct(core.shape, jnp.float32),
            jax.ShapeDtypeStruct((batches, rank, groups * mine), jnp.float32),
        ),
        out_specs=(
            pl.BlockSpec(memory_space=pl.ANY),
            pl.BlockSpec(memory_space=pltpu.VMEM),
            pl.BlockSpec(memory_space=pltpu.VMEM),
        ),
        scratch_shapes=[pltpu.VMEM(basis.shape, jnp.float32), pltpu.SemaphoreType.DMA],
        compiler_params=SMALL_GRANT,
    )(packed, core, basis, received)


def body(basis, core, snapshots):
    batches, mine, dofs = snapshots.shape
    grp = lax.axis_size("grp")
    pieces = snapshots.reshape(batches, mine, grp, dofs // grp).transpose(2, 0, 1, 3)
    received = exchange(pieces, "grp")
    packed = total_over_all(gram_call(received, basis))
    return update_call(packed, core, basis, received)


def solution(mesh):
    finer = Mesh(
        mesh.devices.reshape(4, 16, 2, mesh.shape["grp"]), ("rows_0", "rows_1", "rows_2", "grp")
    )
    return jax.shard_map(
        body,
        mesh=finer,
        in_specs=(P(None, ROWS_GRP), P(), P(None, "grp", ROWS)),
        out_specs=(P(None, ROWS_GRP), P(), P()),
        check_vma=False,
    )
```

```python
import jax
import jax.numpy as jnp
from jax import lax
from jax.experimental import pallas as pl
from jax.experimental.pallas import tpu as pltpu
from jax.sharding import Mesh
from jax.sharding import PartitionSpec as P

BATCHES = 4
ROWS_GRP = ("rows_0", "rows_1", "rows_2", "grp")
ROWS = ("rows_0", "rows_1", "rows_2")
NEAR = ("rows_0", "rows_2", "grp")
FAR = "rows_1"
LANES = 128
SUB = 8
CHUNKS = 1
SMALL_GRANT = pltpu.CompilerParams(vmem_limit_bytes=8 * 2**20)

epsilon = 1e-06


def exchange(parts, axis):
    return lax.all_to_all(parts, axis, split_axis=0, concat_axis=0, tiled=True)


def total_over_all(packed):
    near = lax.axis_size(NEAR)
    far = lax.axis_size(FAR)
    rows, lanes = packed.shape
    piece = exchange(packed.reshape(near, rows // near, lanes), NEAR).sum(axis=0)
    piece = exchange(jnp.broadcast_to(piece, (far, *piece.shape)), FAR).sum(axis=0)
    return exchange(jnp.broadcast_to(piece, (near, *piece.shape)), NEAR).reshape(rows, lanes)


def dot(left, right, contract=(1, 0)):
    return lax.dot_general(
        left,
        right,
        (((contract[0],), (contract[1],)), ((), ())),
        precision=lax.Precision.HIGHEST,
        preferred_element_type=jnp.float32,
    )


def dot_short(left, right, contract=(1, 0)):
    return lax.dot_general(
        left,
        right,
        (((contract[0],), (contract[1],)), ((), ())),
        preferred_element_type=jnp.float32,
    )


def three_parts(values):
    high = values.astype(jnp.bfloat16)
    rest = values - high.astype(jnp.float32)
    middle = rest.astype(jnp.bfloat16)
    low = (rest - middle.astype(jnp.float32)).astype(jnp.bfloat16)
    return high, middle, low


def by_batch(received):
    groups, batches, cols, dofs = received.shape
    return [
        jnp.concatenate([received[g, b] for g in range(groups)], axis=0) for b in range(batches)
    ]


def gram_kernel(received_ref, basis_ref, packed_ref, held_ref):
    raw = jnp.concatenate(by_batch(received_ref[...]), axis=0)
    parts = jnp.concatenate(three_parts(basis_ref[...]), axis=0)
    cols = raw.shape[0]
    held_ref[:cols] = raw
    held_ref[cols:] = parts
    rank = basis_ref.shape[0]
    raw_gram = dot_short(raw, raw, (1, 1))
    cross = dot_short(parts, raw, (1, 1))
    square = dot_short(parts, parts, (1, 1))
    cross = cross[2 * rank :] + cross[rank : 2 * rank] + cross[:rank]
    square = square[2 * rank :] + square[rank : 2 * rank] + square[:rank]
    square = square[:, 2 * rank :] + square[:, rank : 2 * rank] + square[:, :rank]
    step = cols // BATCHES
    packed_ref[0:step] = raw_gram[0:step]
    packed_ref[step : 2 * step] = jnp.concatenate(
        [raw_gram[3 * step :, 3 * step :], raw_gram[step : 2 * step, step:]], axis=1
    )
    packed_ref[2 * step : 3 * step] = jnp.concatenate(
        [square, raw_gram[2 * step : 3 * step, step:]], axis=1
    )
    packed_ref[3 * step :] = cross


def eliminate(matrix, want_inverse):
    order = matrix.shape[0]
    tiles = order // SUB
    row = lax.broadcasted_iota(jnp.int32, (SUB, order), 0)
    lane = lax.broadcasted_iota(jnp.int32, (SUB, order), 1)
    inverse = [jnp.where(row + SUB * g == lane, 1.0, 0.0) for g in range(tiles)]
    lower = [jnp.zeros((SUB, order), jnp.float32) for g in range(tiles)]
    scale = [jnp.zeros((SUB, order), jnp.float32) for g in range(tiles)]

    def spread(tile, k):
        return jnp.broadcast_to(tile[k : k + 1], (SUB, order))

    columns = {
        (m, g): jnp.broadcast_to(matrix[SUB * g : SUB * g + SUB, m : m + 1], (SUB, order))
        for m in range(order)
        for g in range(m // SUB, tiles)
    }
    for j in range(order):
        p, k = divmod(j, SUB)
        pivot = spread(columns[j, p], k)
        root = lax.rsqrt(pivot)
        recip = 1.0 / pivot
        scale[p] = jnp.where(row == k, root, scale[p])
        factors = {g: columns[j, g] * recip for g in range(p, tiles)}
        factors[p] = jnp.where(row > k, factors[p], 0.0)
        if not want_inverse:
            for g in range(p, tiles):
                part = columns[j, g] * root
                if g == p:
                    part = jnp.where(row >= k, part, 0.0)
                lower[g] = jnp.where(lane == j, part, lower[g])
        for m in range(j + 1, order):
            top = spread(columns[j, m // SUB], m % SUB)
            for g in range(m // SUB, tiles):
                columns[m, g] = columns[m, g] - factors[g] * top
        if want_inverse:
            top = spread(inverse[p], k)
            for g in range(p, tiles):
                inverse[g] = inverse[g] - factors[g] * top
    if want_inverse:
        return jnp.concatenate([inverse[g] * scale[g] for g in range(tiles)], axis=0)
    return jnp.concatenate(lower, axis=0)


def update_kernel(
    packed_ref, core_ref, held_ref, new_basis_ref, new_core_ref, firsts_ref, made_ref, sent
):
    cols = packed_ref.shape[1]
    step = cols // BATCHES
    rank = core_ref.shape[0]
    eye = jnp.where(
        lax.broadcasted_iota(jnp.int32, (step, step), 0) == lax.broadcasted_iota(jnp.int32, (step, step), 1), 1.0, 0.0
    )
    rows = [packed_ref[step * b : step * b + step] for b in range(BATCHES - 1)]
    cross = packed_ref[3 * step :]
    grams = [rows[b][:, step * b : step * b + step] for b in range(BATCHES - 1)] + [rows[1][:, :step]]
    scales = [lax.rsqrt(jnp.sum(g * eye, axis=0, keepdims=True) + epsilon) for g in grams]
    gram_basis = rows[2][:, :rank]
    first = cross[:, :step] * scales[0]
    root = core_ref[...]
    energy = dot(root, root, (1, 1))
    of_basis = None
    of_raw = None
    for b in range(BATCHES):
        more = b + 1 < BATCHES
        scale = scales[b]
        firsts_ref[b] = first
        defect = eye - gram_basis
        second = dot(defect, first)
        total = first + second
        weight = total * scale
        rest = dot(defect, second)
        minus_square = dot(-total, total, (1, 1))
        total_raw = dot(weight, grams[b]) * scale
        total_gram = (
            total_raw - dot(dot(total, first, (1, 1)), total) + dot(minus_square, rest)
        )
        leading = energy - minus_square
        square = dot(leading, leading) + dot(total_gram, total, (1, 1))
        tail = dot(leading, total)
        grown = dot(leading, root)
        if more:
            mixed = dot(energy, cross) - dot(-weight, rows[b])
            upcoming = mixed[:, step * b + step : step * b + 2 * step]
            held = dot(energy, first)
            mixed_gram = (
                dot(dot(energy, gram_basis), energy)
                + dot(held, total, (1, 1))
                + dot(total, held, (1, 1))
                + dot(total_raw, total, (1, 1))
            )
        if b:
            of_basis = dot(energy, of_basis)
            if not more:
                of_basis = jnp.concatenate([of_basis] * 3, axis=1)
            of_raw = jnp.concatenate([dot(energy, of_raw), weight], axis=1)
        else:
            of_basis = energy
            of_raw = weight
        inverse = eliminate(square, True)
        root = dot(inverse, grown)
        tail = dot(inverse, tail) + dot(inverse, total_gram)
        if more:
            first = dot(inverse, upcoming) * scales[b + 1]
            gram_basis = dot(dot(inverse, mixed_gram), inverse, (1, 1))
            cross = dot(inverse, mixed)
        energy = dot(root, root, (1, 1)) + dot(tail, tail, (1, 1))
        if more:
            root = jnp.concatenate([root, tail], axis=1)
        of_basis = dot(inverse, of_basis)
        of_raw = dot(inverse, of_raw)
    basis_parts = three_parts(of_basis)
    part = lax.broadcasted_iota(jnp.int32, of_basis.shape, 1) // rank
    basis_parts = [
        jnp.where(part < 3 - n, basis_parts[n].astype(jnp.float32), 0.0).astype(jnp.bfloat16) for n in range(3)
    ]
    mixing = jnp.concatenate(
        [jnp.concatenate(three_parts(of_raw), axis=0), jnp.concatenate(basis_parts, axis=0)], axis=1
    )
    chunk = made_ref.shape[2]
    copies = []
    for n in range(CHUNKS):
        made = dot_short(mixing, held_ref[:, chunk * n : chunk * n + chunk])
        made_ref[n] = made[2 * rank :] + made[rank : 2 * rank] + made[:rank]
        copies.append(
            pltpu.make_async_copy(
                made_ref.at[n], new_basis_ref.at[:, pl.ds(chunk * n, chunk)], sent.at[n]
            )
        )
        copies[n].start()
    new_core_ref[...] = eliminate(energy, False)
    for out in copies:
        out.wait()


def gram_call(received, basis):
    groups, batches, mine, dofs = received.shape
    return pl.pallas_call(
        gram_kernel,
        out_shape=(
            jax.ShapeDtypeStruct((3 * groups * mine + basis.shape[0], LANES), jnp.float32),
            jax.ShapeDtypeStruct((batches * groups * mine + 3 * basis.shape[0], dofs), jnp.bfloat16),
        ),
        compiler_params=SMALL_GRANT,
    )(received, basis)


def update_call(packed, core, held):
    rank = core.shape[0]
    dofs = held.shape[1]
    step = packed.shape[1] // BATCHES
    return pl.pallas_call(
        update_kernel,
        out_shape=(
            jax.ShapeDtypeStruct((rank, dofs), jnp.float32),
            jax.ShapeDtypeStruct((rank, rank), jnp.float32),
            jax.ShapeDtypeStruct((BATCHES, rank, step), jnp.float32),
        ),
        out_specs=(
            pl.BlockSpec(memory_space=pl.ANY),
            pl.BlockSpec(memory_space=pltpu.VMEM),
            pl.BlockSpec(memory_space=pltpu.VMEM),
        ),
        scratch_shapes=[
            pltpu.VMEM((CHUNKS, rank, dofs // CHUNKS), jnp.float32),
            pltpu.SemaphoreType.DMA((CHUNKS,)),
        ],
        compiler_params=SMALL_GRANT,
    )(packed, core, held)


def body(basis, core, snapshots):
    batches, mine, dofs = snapshots.shape
    grp = lax.axis_size("grp")
    pieces = snapshots.reshape(batches, mine, grp, dofs // grp).transpose(2, 0, 1, 3)
    packed, held = gram_call(exchange(pieces, "grp"), basis)
    return update_call(total_over_all(packed), core, held)


def solution(mesh):
    finer = Mesh(
        mesh.devices.reshape(4, 16, 2, mesh.shape["grp"]), ("rows_0", "rows_1", "rows_2", "grp")
    )
    return jax.shard_map(
        body,
        mesh=finer,
        in_specs=(P(None, ROWS_GRP), P(), P(None, "grp", ROWS)),
        out_specs=(P(None, ROWS_GRP), P(), P()),
        check_vma=False,
    )
```

```python
import jax
import jax.numpy as jnp
from jax import lax
from jax.experimental import pallas as pl
from jax.experimental.pallas import tpu as pltpu
from jax.sharding import Mesh
from jax.sharding import PartitionSpec as P

BATCHES = 4
ROWS_GRP = ("rows_0", "rows_1", "rows_2", "grp")
ROWS = ("rows_0", "rows_1", "rows_2")
NEAR = ("rows_0", "rows_2", "grp")
FAR = "rows_1"
LANES = 128
SUB = 8
CHUNKS = 2
SMALL_GRANT = pltpu.CompilerParams(vmem_limit_bytes=8 * 2**20)

epsilon = 1e-06


def exchange(parts, axis):
    return lax.all_to_all(parts, axis, split_axis=0, concat_axis=0, tiled=True)


def total_over_all(packed):
    near = lax.axis_size(NEAR)
    far = lax.axis_size(FAR)
    rows, lanes = packed.shape
    piece = exchange(packed.reshape(near, rows // near, lanes), NEAR).sum(axis=0)
    piece = exchange(jnp.broadcast_to(piece, (far, *piece.shape)), FAR).sum(axis=0)
    return exchange(jnp.broadcast_to(piece, (near, *piece.shape)), NEAR).reshape(rows, lanes)


def dot(left, right, contract=(1, 0)):
    rows = left.shape[0]
    lefts = three_parts(left)
    high, middle, low = three_parts(right)
    first = dot_short(jnp.concatenate(lefts, axis=0), high, contract)
    second = dot_short(jnp.concatenate(lefts[:2], axis=0), middle, contract)
    third = dot_short(lefts[0], low, contract)
    small = first[2 * rows :] + second[rows:] + third
    return first[:rows] + ((first[rows : 2 * rows] + second[:rows]) + small)


def dot_short(left, right, contract=(1, 0)):
    return lax.dot_general(
        left,
        right,
        (((contract[0],), (contract[1],)), ((), ())),
        preferred_element_type=jnp.float32,
    )


def dot_middle(left, right):
    rows = left.shape[0]
    high, middle, low = three_parts(left)
    right_high, right_middle, right_low = three_parts(right)
    first = dot_short(jnp.concatenate([high, middle], axis=0), right_high)
    return first[:rows] + (first[rows:] + dot_short(high, right_middle))


def three_parts(values):
    high = values.astype(jnp.bfloat16)
    rest = values - high.astype(jnp.float32)
    middle = rest.astype(jnp.bfloat16)
    low = (rest - middle.astype(jnp.float32)).astype(jnp.bfloat16)
    return high, middle, low


def by_batch(received):
    groups, batches, cols, dofs = received.shape
    return [
        jnp.concatenate([received[g, b] for g in range(groups)], axis=0) for b in range(batches)
    ]


def gram_kernel(received_ref, basis_ref, packed_ref, held_ref):
    raw = jnp.concatenate(by_batch(received_ref[...]), axis=0)
    parts = jnp.concatenate(three_parts(basis_ref[...]), axis=0)
    cols = raw.shape[0]
    held_ref[:cols] = raw
    held_ref[cols:] = parts
    rank = basis_ref.shape[0]
    raw_gram = dot_short(raw, raw, (1, 1))
    cross = dot_short(parts, raw, (1, 1))
    square = dot_short(parts, parts, (1, 1))
    cross = cross[2 * rank :] + cross[rank : 2 * rank] + cross[:rank]
    square = square[2 * rank :] + square[rank : 2 * rank] + square[:rank]
    square = square[:, 2 * rank :] + square[:, rank : 2 * rank] + square[:, :rank]
    step = cols // BATCHES
    packed_ref[0:step] = raw_gram[0:step]
    packed_ref[step : 2 * step] = jnp.concatenate(
        [raw_gram[3 * step :, 3 * step :], raw_gram[step : 2 * step, step:]], axis=1
    )
    packed_ref[2 * step : 3 * step] = jnp.concatenate(
        [square, raw_gram[2 * step : 3 * step, step:]], axis=1
    )
    packed_ref[3 * step :] = cross


def eliminate(matrix, rights=(), want_inverse=True):
    order = matrix.shape[0]
    tiles = order // SUB
    row = lax.broadcasted_iota(jnp.int32, (SUB, order), 0)
    lane = lax.broadcasted_iota(jnp.int32, (SUB, order), 1)
    solved = [[r[SUB * g : SUB * g + SUB] for g in range(tiles)] for r in rights]
    if want_inverse:
        solved.insert(0, [jnp.where(row + SUB * g == lane, 1.0, 0.0) for g in range(tiles)])
    lower = [jnp.zeros((SUB, order), jnp.float32) for g in range(tiles)]
    scale = [jnp.zeros((SUB, order), jnp.float32) for g in range(tiles)]

    def spread(tile, k):
        return jnp.broadcast_to(tile[k : k + 1], tile.shape)

    columns = {
        (m, g): jnp.broadcast_to(matrix[SUB * g : SUB * g + SUB, m : m + 1], (SUB, order))
        for m in range(order)
        for g in range(m // SUB, tiles)
    }
    for j in range(order):
        p, k = divmod(j, SUB)
        pivot = spread(columns[j, p], k)
        root = lax.rsqrt(pivot)
        recip = 1.0 / pivot
        scale[p] = jnp.where(row == k, root, scale[p])
        factors = {g: columns[j, g] * recip for g in range(p, tiles)}
        factors[p] = jnp.where(row > k, factors[p], 0.0)
        if not want_inverse:
            for g in range(p, tiles):
                part = columns[j, g] * root
                if g == p:
                    part = jnp.where(row >= k, part, 0.0)
                lower[g] = jnp.where(lane == j, part, lower[g])
        for m in range(j + 1, order):
            top = spread(columns[j, m // SUB], m % SUB)
            for g in range(m // SUB, tiles):
                columns[m, g] = columns[m, g] - factors[g] * top
        for right in solved:
            top = spread(right[p], k)
            for g in range(p, tiles):
                right[g] = right[g] - factors[g] * top
    if not want_inverse:
        return jnp.concatenate(lower, axis=0)
    return [jnp.concatenate([right[g] * scale[g] for g in range(tiles)], axis=0) for right in solved]


def update_kernel(
    packed_ref, core_ref, held_ref, new_basis_ref, new_core_ref, firsts_ref, made_ref, sent
):
    cols = packed_ref.shape[1]
    step = cols // BATCHES
    rank = core_ref.shape[0]
    eye = jnp.where(
        lax.broadcasted_iota(jnp.int32, (step, step), 0) == lax.broadcasted_iota(jnp.int32, (step, step), 1), 1.0, 0.0
    )
    rows = [packed_ref[step * b : step * b + step] for b in range(BATCHES - 1)]
    cross = packed_ref[3 * step :]
    grams = [rows[b][:, step * b : step * b + step] for b in range(BATCHES - 1)] + [rows[1][:, :step]]
    scales = [lax.rsqrt(jnp.sum(g * eye, axis=0, keepdims=True) + epsilon) for g in grams]
    gram_basis = rows[2][:, :rank]
    first = cross[:, :step] * scales[0]
    root = core_ref[...]
    energy = dot(root, root, (1, 1))
    of_basis = None
    of_raw = None
    for b in range(BATCHES):
        more = b + 1 < BATCHES
        scale = scales[b]
        firsts_ref[b] = first
        defect = eye - gram_basis
        second = dot_middle(defect, first)
        total = first + second
        weight = total * scale
        rest = dot_middle(defect, second)
        minus_square = dot(-total, total, (1, 1))
        total_raw = dot(weight, grams[b]) * scale
        total_gram = (
            total_raw - dot(dot(total, first, (1, 1)), total) + dot_middle(minus_square, rest)
        )
        leading = energy - minus_square
        square = dot(leading, leading) + dot(total_gram, total, (1, 1))
        tail = dot(leading, total)
        grown = dot(leading, root)
        if more:
            mixed = dot(energy, cross) - dot(-weight, rows[b])
            upcoming = mixed[:, step * b + step : step * b + 2 * step]
            held = dot(energy, first)
            mixed_gram = (
                dot(dot(energy, gram_basis), energy)
                + dot(held, total, (1, 1))
                + dot(total, held, (1, 1))
                + dot(total_raw, total, (1, 1))
            )
        if b:
            of_basis = dot(energy, of_basis)
            if not more:
                of_basis = jnp.concatenate([of_basis] * 3, axis=1)
            of_raw = jnp.concatenate([dot(energy, of_raw), weight], axis=1)
        else:
            of_basis = energy
            of_raw = weight
        (inverse,) = eliminate(square)
        root = dot(inverse, grown)
        tail = dot(inverse, tail) + dot(inverse, total_gram)
        if more:
            first = dot(inverse, upcoming) * scales[b + 1]
            gram_basis = dot(dot(inverse, mixed_gram), inverse, (1, 1))
            cross = dot(inverse, mixed)
        energy = dot(root, root, (1, 1)) + dot(tail, tail, (1, 1))
        if more:
            root = jnp.concatenate([root, tail], axis=1)
        of_basis = dot(inverse, of_basis)
        of_raw = dot(inverse, of_raw)
    basis_parts = three_parts(of_basis)
    part = lax.broadcasted_iota(jnp.int32, of_basis.shape, 1) // rank
    basis_parts = [
        jnp.where(part < 3 - n, basis_parts[n].astype(jnp.float32), 0.0).astype(jnp.bfloat16) for n in range(3)
    ]
    mixing = jnp.concatenate(
        [jnp.concatenate(three_parts(of_raw), axis=0), jnp.concatenate(basis_parts, axis=0)], axis=1
    )
    chunk = made_ref.shape[2]
    copies = []
    for n in range(CHUNKS):
        made = dot_short(mixing, held_ref[:, chunk * n : chunk * n + chunk])
        made_ref[n] = made[2 * rank :] + made[rank : 2 * rank] + made[:rank]
        copies.append(
            pltpu.make_async_copy(
                made_ref.at[n], new_basis_ref.at[:, pl.ds(chunk * n, chunk)], sent.at[n]
            )
        )
        copies[n].start()
    new_core_ref[...] = eliminate(energy, want_inverse=False)
    for out in copies:
        out.wait()


def gram_call(received, basis):
    groups, batches, mine, dofs = received.shape
    return pl.pallas_call(
        gram_kernel,
        out_shape=(
            jax.ShapeDtypeStruct((3 * groups * mine + basis.shape[0], LANES), jnp.float32),
            jax.ShapeDtypeStruct((batches * groups * mine + 3 * basis.shape[0], dofs), jnp.bfloat16),
        ),
        compiler_params=SMALL_GRANT,
    )(received, basis)


def update_call(packed, core, held):
    rank = core.shape[0]
    dofs = held.shape[1]
    step = packed.shape[1] // BATCHES
    return pl.pallas_call(
        update_kernel,
        out_shape=(
            jax.ShapeDtypeStruct((rank, dofs), jnp.float32),
            jax.ShapeDtypeStruct((rank, rank), jnp.float32),
            jax.ShapeDtypeStruct((BATCHES, rank, step), jnp.float32),
        ),
        out_specs=(
            pl.BlockSpec(memory_space=pl.ANY),
            pl.BlockSpec(memory_space=pltpu.VMEM),
            pl.BlockSpec(memory_space=pltpu.VMEM),
        ),
        scratch_shapes=[
            pltpu.VMEM((CHUNKS, rank, dofs // CHUNKS), jnp.float32),
            pltpu.SemaphoreType.DMA((CHUNKS,)),
        ],
        compiler_params=SMALL_GRANT,
    )(packed, core, held)


def body(basis, core, snapshots):
    batches, mine, dofs = snapshots.shape
    grp = lax.axis_size("grp")
    pieces = snapshots.reshape(batches, mine, grp, dofs // grp).transpose(2, 0, 1, 3)
    packed, held = gram_call(exchange(pieces, "grp"), basis)
    return update_call(total_over_all(packed), core, held)


def solution(mesh):
    finer = Mesh(
        mesh.devices.reshape(4, 16, 2, mesh.shape["grp"]), ("rows_0", "rows_1", "rows_2", "grp")
    )
    return jax.shard_map(
        body,
        mesh=finer,
        in_specs=(P(None, ROWS_GRP), P(), P(None, "grp", ROWS)),
        out_specs=(P(None, ROWS_GRP), P(), P()),
        check_vma=False,
    )
```

```python
import jax
import jax.numpy as jnp
from jax import lax
from jax.experimental import pallas as pl
from jax.experimental.pallas import tpu as pltpu
from jax.sharding import Mesh
from jax.sharding import PartitionSpec as P

BATCHES = 4
ROWS_GRP = ("rows_0", "rows_1", "rows_2", "grp")
ROWS = ("rows_0", "rows_1", "rows_2")
NEAR = ("rows_0", "grp")
CORE = "rows_2"
FAR = "rows_1"
LANES = 128
SUB = 8
CHUNKS = 2
SMALL_GRANT = pltpu.CompilerParams(vmem_limit_bytes=8 * 2**20)

epsilon = 1e-06


def exchange(parts, axis):
    return lax.all_to_all(parts, axis, split_axis=0, concat_axis=0, tiled=True)


def total_over_all(packed):
    near = lax.axis_size(NEAR)
    cores = lax.axis_size(CORE)
    far = lax.axis_size(FAR)
    rows, lanes = packed.shape
    piece = exchange(packed.reshape(near * cores, rows // (near * cores), lanes), (*NEAR, CORE)).sum(axis=0)
    pieces = exchange(jnp.broadcast_to(piece, (far * cores, *piece.shape)), (FAR, CORE))
    pair = pieces.reshape(far, cores, *piece.shape).sum(axis=0).reshape(rows // near, lanes)
    return exchange(jnp.broadcast_to(pair, (near, *pair.shape)), NEAR).reshape(rows, lanes)


def dot(left, right, contract=(1, 0)):
    rows = left.shape[0]
    lefts = three_parts(left)
    high, middle, low = three_parts(right)
    first = dot_short(jnp.concatenate(lefts, axis=0), high, contract)
    second = dot_short(jnp.concatenate(lefts[:2], axis=0), middle, contract)
    third = dot_short(lefts[0], low, contract)
    small = first[2 * rows :] + second[rows:] + third
    return first[:rows] + ((first[rows : 2 * rows] + second[:rows]) + small)


def dot_short(left, right, contract=(1, 0)):
    return lax.dot_general(
        left,
        right,
        (((contract[0],), (contract[1],)), ((), ())),
        preferred_element_type=jnp.float32,
    )


def dot_middle(left, right):
    rows = left.shape[0]
    high, middle, low = three_parts(left)
    right_high, right_middle, right_low = three_parts(right)
    first = dot_short(jnp.concatenate([high, middle], axis=0), right_high)
    return first[:rows] + (first[rows:] + dot_short(high, right_middle))


def three_parts(values):
    high = values.astype(jnp.bfloat16)
    rest = values - high.astype(jnp.float32)
    middle = rest.astype(jnp.bfloat16)
    low = (rest - middle.astype(jnp.float32)).astype(jnp.bfloat16)
    return high, middle, low


def by_batch(received):
    groups, batches, cols, dofs = received.shape
    return [
        jnp.concatenate([received[g, b] for g in range(groups)], axis=0) for b in range(batches)
    ]


def gram_kernel(received_ref, basis_ref, packed_ref, held_ref):
    raw = jnp.concatenate(by_batch(received_ref[...]), axis=0)
    parts = jnp.concatenate(three_parts(basis_ref[...]), axis=0)
    cols = raw.shape[0]
    held_ref[:cols] = raw
    held_ref[cols:] = parts
    rank = basis_ref.shape[0]
    raw_gram = dot_short(raw, raw, (1, 1))
    cross = dot_short(parts, raw, (1, 1))
    square = dot_short(parts, parts, (1, 1))
    cross = cross[2 * rank :] + cross[rank : 2 * rank] + cross[:rank]
    square = square[2 * rank :] + square[rank : 2 * rank] + square[:rank]
    square = square[:, 2 * rank :] + square[:, rank : 2 * rank] + square[:, :rank]
    step = cols // BATCHES
    packed_ref[0:step] = raw_gram[0:step]
    packed_ref[step : 2 * step] = jnp.concatenate(
        [raw_gram[3 * step :, 3 * step :], raw_gram[step : 2 * step, step:]], axis=1
    )
    packed_ref[2 * step : 3 * step] = jnp.concatenate(
        [square, raw_gram[2 * step : 3 * step, step:]], axis=1
    )
    packed_ref[3 * step :] = cross


def eliminate(matrix, rights=(), want_inverse=True):
    order = matrix.shape[0]
    tiles = order // SUB
    row = lax.broadcasted_iota(jnp.int32, (SUB, order), 0)
    lane = lax.broadcasted_iota(jnp.int32, (SUB, order), 1)
    solved = [[r[SUB * g : SUB * g + SUB] for g in range(tiles)] for r in rights]
    if want_inverse:
        solved.insert(0, [jnp.where(row + SUB * g == lane, 1.0, 0.0) for g in range(tiles)])
    lower = [jnp.zeros((SUB, order), jnp.float32) for g in range(tiles)]
    scale = [jnp.zeros((SUB, order), jnp.float32) for g in range(tiles)]

    def spread(tile, k):
        return jnp.broadcast_to(tile[k : k + 1], tile.shape)

    columns = {
        (m, g): jnp.broadcast_to(matrix[SUB * g : SUB * g + SUB, m : m + 1], (SUB, order))
        for m in range(order)
        for g in range(m // SUB, tiles)
    }
    for j in range(order):
        p, k = divmod(j, SUB)
        pivot = spread(columns[j, p], k)
        root = lax.rsqrt(pivot)
        recip = 1.0 / pivot
        scale[p] = jnp.where(row == k, root, scale[p])
        factors = {g: columns[j, g] * recip for g in range(p, tiles)}
        factors[p] = jnp.where(row > k, factors[p], 0.0)
        if not want_inverse:
            for g in range(p, tiles):
                part = columns[j, g] * root
                if g == p:
                    part = jnp.where(row >= k, part, 0.0)
                lower[g] = jnp.where(lane == j, part, lower[g])
        for m in range(j + 1, order):
            top = spread(columns[j, m // SUB], m % SUB)
            for g in range(m // SUB, tiles):
                columns[m, g] = columns[m, g] - factors[g] * top
        for right in solved:
            top = spread(right[p], k)
            for g in range(p, tiles):
                right[g] = right[g] - factors[g] * top
    if not want_inverse:
        return jnp.concatenate(lower, axis=0)
    return [jnp.concatenate([right[g] * scale[g] for g in range(tiles)], axis=0) for right in solved]


def update_kernel(
    packed_ref, core_ref, held_ref, new_basis_ref, new_core_ref, firsts_ref, made_ref, sent
):
    cols = packed_ref.shape[1]
    step = cols // BATCHES
    rank = core_ref.shape[0]
    eye = jnp.where(
        lax.broadcasted_iota(jnp.int32, (step, step), 0) == lax.broadcasted_iota(jnp.int32, (step, step), 1), 1.0, 0.0
    )
    rows = [packed_ref[step * b : step * b + step] for b in range(BATCHES - 1)]
    cross = packed_ref[3 * step :]
    grams = [rows[b][:, step * b : step * b + step] for b in range(BATCHES - 1)] + [rows[1][:, :step]]
    scales = [lax.rsqrt(jnp.sum(g * eye, axis=0, keepdims=True) + epsilon) for g in grams]
    gram_basis = rows[2][:, :rank]
    first = cross[:, :step] * scales[0]
    root = core_ref[...]
    energy = dot(root, root, (1, 1))
    of_basis = None
    of_raw = None
    for b in range(BATCHES):
        more = b + 1 < BATCHES
        scale = scales[b]
        firsts_ref[b] = first
        defect = eye - gram_basis
        second = dot_middle(defect, first)
        total = first + second
        weight = total * scale
        rest = dot_middle(defect, second)
        minus_square = dot(-total, total, (1, 1))
        total_raw = dot(weight, grams[b]) * scale
        total_gram = (
            total_raw - dot(dot(total, first, (1, 1)), total) + dot_middle(minus_square, rest)
        )
        leading = energy - minus_square
        square = dot(leading, leading) + dot(total_gram, total, (1, 1))
        tail = dot(leading, total)
        grown = dot(leading, root)
        if more:
            mixed = dot(energy, cross) - dot(-weight, rows[b])
            upcoming = mixed[:, step * b + step : step * b + 2 * step]
            held = dot(energy, first)
            mixed_gram = (
                dot(dot(energy, gram_basis), energy)
                + dot(held, total, (1, 1))
                + dot(total, held, (1, 1))
                + dot(total_raw, total, (1, 1))
            )
        if b:
            of_basis = dot(energy, of_basis)
            if not more:
                of_basis = jnp.concatenate([of_basis] * 3, axis=1)
            of_raw = jnp.concatenate([dot(energy, of_raw), weight], axis=1)
        else:
            of_basis = energy
            of_raw = weight
        (inverse,) = eliminate(square)
        root = dot(inverse, grown)
        tail = dot(inverse, tail) + dot(inverse, total_gram)
        if more:
            first = dot(inverse, upcoming) * scales[b + 1]
            gram_basis = dot(dot(inverse, mixed_gram), inverse, (1, 1))
            cross = dot(inverse, mixed)
        energy = dot(root, root, (1, 1)) + dot(tail, tail, (1, 1))
        if more:
            root = jnp.concatenate([root, tail], axis=1)
        of_basis = dot(inverse, of_basis)
        of_raw = dot(inverse, of_raw)
    basis_parts = three_parts(of_basis)
    part = lax.broadcasted_iota(jnp.int32, of_basis.shape, 1) // rank
    basis_parts = [
        jnp.where(part < 3 - n, basis_parts[n].astype(jnp.float32), 0.0).astype(jnp.bfloat16) for n in range(3)
    ]
    mixing = jnp.concatenate(
        [jnp.concatenate(three_parts(of_raw), axis=0), jnp.concatenate(basis_parts, axis=0)], axis=1
    )
    chunk = made_ref.shape[2]
    copies = []
    for n in range(CHUNKS):
        made = dot_short(mixing, held_ref[:, chunk * n : chunk * n + chunk])
        made_ref[n] = made[2 * rank :] + made[rank : 2 * rank] + made[:rank]
        copies.append(
            pltpu.make_async_copy(
                made_ref.at[n], new_basis_ref.at[:, pl.ds(chunk * n, chunk)], sent.at[n]
            )
        )
        copies[n].start()
    new_core_ref[...] = eliminate(energy, want_inverse=False)
    for out in copies:
        out.wait()


def gram_call(received, basis):
    groups, batches, mine, dofs = received.shape
    return pl.pallas_call(
        gram_kernel,
        out_shape=(
            jax.ShapeDtypeStruct((3 * groups * mine + basis.shape[0], LANES), jnp.float32),
            jax.ShapeDtypeStruct((batches * groups * mine + 3 * basis.shape[0], dofs), jnp.bfloat16),
        ),
        compiler_params=SMALL_GRANT,
    )(received, basis)


def update_call(packed, core, held):
    rank = core.shape[0]
    dofs = held.shape[1]
    step = packed.shape[1] // BATCHES
    return pl.pallas_call(
        update_kernel,
        out_shape=(
            jax.ShapeDtypeStruct((rank, dofs), jnp.float32),
            jax.ShapeDtypeStruct((rank, rank), jnp.float32),
            jax.ShapeDtypeStruct((BATCHES, rank, step), jnp.float32),
        ),
        out_specs=(
            pl.BlockSpec(memory_space=pl.ANY),
            pl.BlockSpec(memory_space=pltpu.VMEM),
            pl.BlockSpec(memory_space=pltpu.VMEM),
        ),
        scratch_shapes=[
            pltpu.VMEM((CHUNKS, rank, dofs // CHUNKS), jnp.float32),
            pltpu.SemaphoreType.DMA((CHUNKS,)),
        ],
        compiler_params=SMALL_GRANT,
    )(packed, core, held)


def body(basis, core, snapshots):
    batches, mine, dofs = snapshots.shape
    grp = lax.axis_size("grp")
    pieces = snapshots.reshape(batches, mine, grp, dofs // grp).transpose(2, 0, 1, 3)
    packed, held = gram_call(exchange(pieces, "grp"), basis)
    return update_call(total_over_all(packed), core, held)


def solution(mesh):
    finer = Mesh(
        mesh.devices.reshape(4, 16, 2, mesh.shape["grp"]), ("rows_0", "rows_1", "rows_2", "grp")
    )
    return jax.shard_map(
        body,
        mesh=finer,
        in_specs=(P(None, ROWS_GRP), P(), P(None, "grp", ROWS)),
        out_specs=(P(None, ROWS_GRP), P(), P()),
        check_vma=False,
    )
```

```python
import jax
import jax.numpy as jnp
from jax import lax
from jax.experimental import pallas as pl
from jax.experimental.pallas import tpu as pltpu
from jax.sharding import Mesh
from jax.sharding import PartitionSpec as P

BATCHES = 4
ROWS_GRP = ("rows_0", "rows_1", "rows_2", "grp")
ROWS = ("rows_0", "rows_1", "rows_2")
NEAR = ("rows_0", "rows_2", "grp")
FAR = "rows_1"
LANES = 128
SUB = 8
CHUNKS = 2
SMALL_GRANT = pltpu.CompilerParams(vmem_limit_bytes=8 * 2**20)

epsilon = 1e-06


def exchange(parts, axis):
    return lax.all_to_all(parts, axis, split_axis=0, concat_axis=0, tiled=True)


def total_over_all(packed):
    near = lax.axis_size(NEAR)
    far = lax.axis_size(FAR)
    rows, lanes = packed.shape
    piece = exchange(packed.reshape(near, rows // near, lanes), NEAR).sum(axis=0)
    piece = exchange(jnp.broadcast_to(piece, (far, *piece.shape)), FAR).sum(axis=0)
    return exchange(jnp.broadcast_to(piece, (near, *piece.shape)), NEAR).reshape(rows, lanes)


def dot(left, right, contract=(1, 0)):
    rows = left.shape[0]
    lefts = three_parts(left)
    high, middle, low = three_parts(right)
    first = dot_short(jnp.concatenate(lefts, axis=0), high, contract)
    second = dot_short(jnp.concatenate(lefts[:2], axis=0), middle, contract)
    third = dot_short(lefts[0], low, contract)
    small = first[2 * rows :] + second[rows:] + third
    return first[:rows] + ((first[rows : 2 * rows] + second[:rows]) + small)


def dot_short(left, right, contract=(1, 0)):
    return lax.dot_general(
        left,
        right,
        (((contract[0],), (contract[1],)), ((), ())),
        preferred_element_type=jnp.float32,
    )


def dot_middle(left, right):
    rows = left.shape[0]
    high, middle, low = three_parts(left)
    right_high, right_middle, right_low = three_parts(right)
    first = dot_short(jnp.concatenate([high, middle], axis=0), right_high)
    return first[:rows] + (first[rows:] + dot_short(high, right_middle))


def three_parts(values):
    high = values.astype(jnp.bfloat16)
    rest = values - high.astype(jnp.float32)
    middle = rest.astype(jnp.bfloat16)
    low = (rest - middle.astype(jnp.float32)).astype(jnp.bfloat16)
    return high, middle, low


def by_batch(received):
    groups, batches, cols, dofs = received.shape
    return [
        jnp.concatenate([received[g, b] for g in range(groups)], axis=0) for b in range(batches)
    ]


def gram_kernel(received_ref, basis_ref, packed_ref, held_ref):
    raw = jnp.concatenate(by_batch(received_ref[...]), axis=0)
    parts = jnp.concatenate(three_parts(basis_ref[...]), axis=0)
    cols = raw.shape[0]
    held_ref[:cols] = raw
    held_ref[cols:] = parts
    rank = basis_ref.shape[0]
    raw_gram = dot_short(raw, raw, (1, 1))
    cross = dot_short(parts, raw, (1, 1))
    square = dot_short(parts, parts, (1, 1))
    cross = cross[2 * rank :] + cross[rank : 2 * rank] + cross[:rank]
    square = square[2 * rank :] + square[rank : 2 * rank] + square[:rank]
    square = square[:, 2 * rank :] + square[:, rank : 2 * rank] + square[:, :rank]
    step = cols // BATCHES
    packed_ref[0:step] = raw_gram[0:step]
    packed_ref[step : 2 * step] = jnp.concatenate(
        [raw_gram[3 * step :, 3 * step :], raw_gram[step : 2 * step, step:]], axis=1
    )
    packed_ref[2 * step : 3 * step] = jnp.concatenate(
        [square, raw_gram[2 * step : 3 * step, step:]], axis=1
    )
    packed_ref[3 * step :] = cross


def eliminate(matrix, rights=(), want_inverse=True):
    order = matrix.shape[0]
    tiles = order // SUB
    row = lax.broadcasted_iota(jnp.int32, (SUB, order), 0)
    lane = lax.broadcasted_iota(jnp.int32, (SUB, order), 1)
    solved = [[r[SUB * g : SUB * g + SUB] for g in range(tiles)] for r in rights]
    if want_inverse:
        solved.insert(0, [jnp.where(row + SUB * g == lane, 1.0, 0.0) for g in range(tiles)])
    lower = [jnp.zeros((SUB, order), jnp.float32) for g in range(tiles)]
    scale = [jnp.zeros((SUB, order), jnp.float32) for g in range(tiles)]

    def spread(tile, k):
        return jnp.broadcast_to(tile[k : k + 1], tile.shape)

    half = order // 2
    ahead = half // SUB
    work = [matrix[SUB * g : SUB * g + SUB] for g in range(tiles)]
    columns = {}

    def take(m, g):
        columns[m, g] = jnp.broadcast_to(work[g][:, m : m + 1], (SUB, order))

    for m in range(half):
        for g in range(m // SUB, tiles):
            take(m, g)
    for m in range(half, half + SUB):
        take(m, ahead)
    for j in range(order):
        p, k = divmod(j, SUB)
        if j == half:
            for m in range(half, order):
                for g in range(ahead + 1, tiles):
                    take(m, g)
        pivot = spread(columns[j, p], k)
        root = lax.rsqrt(pivot)
        recip = 1.0 / pivot
        scale[p] = jnp.where(row == k, root, scale[p])
        factors = {g: columns[j, g] * recip for g in range(p, tiles)}
        factors[p] = jnp.where(row > k, factors[p], 0.0)
        if not want_inverse:
            for g in range(p, tiles):
                part = columns[j, g] * root
                if g == p:
                    part = jnp.where(row >= k, part, 0.0)
                lower[g] = jnp.where(lane == j, part, lower[g])
        for m in range(j + 1, half + SUB if j < half else order):
            top = spread(columns[j, m // SUB], m % SUB)
            for g in range(m // SUB, tiles if m < half or j >= half else ahead + 1):
                columns[m, g] = columns[m, g] - factors[g] * top
        if j < half:
            top = spread(work[p], k)
            for g in range(p, tiles):
                work[g] = work[g] - factors[g] * top
        for right in solved:
            top = spread(right[p], k)
            for g in range(p, tiles):
                right[g] = right[g] - factors[g] * top
    if not want_inverse:
        return jnp.concatenate(lower, axis=0)
    return [jnp.concatenate([right[g] * scale[g] for g in range(tiles)], axis=0) for right in solved]


def update_kernel(
    packed_ref, core_ref, held_ref, new_basis_ref, new_core_ref, firsts_ref, made_ref, sent
):
    cols = packed_ref.shape[1]
    step = cols // BATCHES
    rank = core_ref.shape[0]
    eye = jnp.where(
        lax.broadcasted_iota(jnp.int32, (step, step), 0) == lax.broadcasted_iota(jnp.int32, (step, step), 1), 1.0, 0.0
    )
    rows = [packed_ref[step * b : step * b + step] for b in range(BATCHES - 1)]
    cross = packed_ref[3 * step :]
    grams = [rows[b][:, step * b : step * b + step] for b in range(BATCHES - 1)] + [rows[1][:, :step]]
    scales = [lax.rsqrt(jnp.sum(g * eye, axis=0, keepdims=True) + epsilon) for g in grams]
    gram_basis = rows[2][:, :rank]
    first = cross[:, :step] * scales[0]
    root = core_ref[...]
    energy = dot(root, root, (1, 1))
    of_basis = None
    of_raw = None
    for b in range(BATCHES):
        more = b + 1 < BATCHES
        scale = scales[b]
        firsts_ref[b] = first
        defect = eye - gram_basis
        second = dot_middle(defect, first)
        total = first + second
        weight = total * scale
        rest = dot_middle(defect, second)
        minus_square = dot(-total, total, (1, 1))
        total_raw = dot(weight, grams[b]) * scale
        total_gram = (
            total_raw - dot(dot(total, first, (1, 1)), total) + dot_middle(minus_square, rest)
        )
        leading = energy - minus_square
        square = dot(leading, leading) + dot(total_gram, total, (1, 1))
        tail = dot(leading, total)
        grown = dot(leading, root)
        if more:
            mixed = dot(energy, cross) - dot(-weight, rows[b])
            upcoming = mixed[:, step * b + step : step * b + 2 * step]
            held = dot(energy, first)
            mixed_gram = (
                dot(dot(energy, gram_basis), energy)
                + dot(held, total, (1, 1))
                + dot(total, held, (1, 1))
                + dot(total_raw, total, (1, 1))
            )
        if b:
            of_basis = dot(energy, of_basis)
            if not more:
                of_basis = jnp.concatenate([of_basis] * 3, axis=1)
            of_raw = jnp.concatenate([dot(energy, of_raw), weight], axis=1)
        else:
            of_basis = energy
            of_raw = weight
        (inverse,) = eliminate(square)
        root = dot(inverse, grown)
        tail = dot(inverse, tail) + dot(inverse, total_gram)
        if more:
            first = dot(inverse, upcoming) * scales[b + 1]
            gram_basis = dot(dot(inverse, mixed_gram), inverse, (1, 1))
            cross = dot(inverse, mixed)
        energy = dot(root, root, (1, 1)) + dot(tail, tail, (1, 1))
        if more:
            root = jnp.concatenate([root, tail], axis=1)
        of_basis = dot(inverse, of_basis)
        of_raw = dot(inverse, of_raw)
    basis_parts = three_parts(of_basis)
    part = lax.broadcasted_iota(jnp.int32, of_basis.shape, 1) // rank
    basis_parts = [
        jnp.where(part < 3 - n, basis_parts[n].astype(jnp.float32), 0.0).astype(jnp.bfloat16) for n in range(3)
    ]
    mixing = jnp.concatenate(
        [jnp.concatenate(three_parts(of_raw), axis=0), jnp.concatenate(basis_parts, axis=0)], axis=1
    )
    chunk = made_ref.shape[2]
    copies = []
    for n in range(CHUNKS):
        made = dot_short(mixing, held_ref[:, chunk * n : chunk * n + chunk])
        made_ref[n] = made[2 * rank :] + made[rank : 2 * rank] + made[:rank]
        copies.append(
            pltpu.make_async_copy(
                made_ref.at[n], new_basis_ref.at[:, pl.ds(chunk * n, chunk)], sent.at[n]
            )
        )
        copies[n].start()
    new_core_ref[...] = eliminate(energy, want_inverse=False)
    for out in copies:
        out.wait()


def gram_call(received, basis):
    groups, batches, mine, dofs = received.shape
    return pl.pallas_call(
        gram_kernel,
        out_shape=(
            jax.ShapeDtypeStruct((3 * groups * mine + basis.shape[0], LANES), jnp.float32),
            jax.ShapeDtypeStruct((batches * groups * mine + 3 * basis.shape[0], dofs), jnp.bfloat16),
        ),
        compiler_params=SMALL_GRANT,
    )(received, basis)


def update_call(packed, core, held):
    rank = core.shape[0]
    dofs = held.shape[1]
    step = packed.shape[1] // BATCHES
    return pl.pallas_call(
        update_kernel,
        out_shape=(
            jax.ShapeDtypeStruct((rank, dofs), jnp.float32),
            jax.ShapeDtypeStruct((rank, rank), jnp.float32),
            jax.ShapeDtypeStruct((BATCHES, rank, step), jnp.float32),
        ),
        out_specs=(
            pl.BlockSpec(memory_space=pl.ANY),
            pl.BlockSpec(memory_space=pltpu.VMEM),
            pl.BlockSpec(memory_space=pltpu.VMEM),
        ),
        scratch_shapes=[
            pltpu.VMEM((CHUNKS, rank, dofs // CHUNKS), jnp.float32),
            pltpu.SemaphoreType.DMA((CHUNKS,)),
        ],
        compiler_params=SMALL_GRANT,
    )(packed, core, held)


def body(basis, core, snapshots):
    batches, mine, dofs = snapshots.shape
    grp = lax.axis_size("grp")
    pieces = snapshots.reshape(batches, mine, grp, dofs // grp).transpose(2, 0, 1, 3)
    packed, held = gram_call(exchange(pieces, "grp"), basis)
    return update_call(total_over_all(packed), core, held)


def solution(mesh):
    finer = Mesh(
        mesh.devices.reshape(4, 16, 2, mesh.shape["grp"]), ("rows_0", "rows_1", "rows_2", "grp")
    )
    return jax.shard_map(
        body,
        mesh=finer,
        in_specs=(P(None, ROWS_GRP), P(), P(None, "grp", ROWS)),
        out_specs=(P(None, ROWS_GRP), P(), P()),
        check_vma=False,
    )
```
